256 devices in a mesh: gx: 8 (over y, core), gy: 8 (over z), gz: 4 (over x).
Axes of the slice: x: 4, y: 4, z: 8, core: 2. Of those that a mesh axis runs over, the one named last changes fastest.
Arguments:
- blocks: bfloat16 [1536, 64, 4096], P(('gx', 'gy', 'gz')), may hold values from -6 to 6
- ownership: int32 [1536, 3], P(('gx', 'gy', 'gz')), may hold values from -1 to 15, as said below
- basis_rows: bfloat16 [1024, 48], replicated, may hold values from -0.1875 to 0.1875
Outputs:
- gram_matrix: float32 [1024, 1024], P(('gx', 'gy', 'gz'))
The draws below stay inside these ranges and needn't reach their ends.
Inputs may be any that keep to these rules, and one draw needn't show every extreme that they name: `ownership`: row d * 6 + s is slot s of device d in mesh order. Each row is a block triple (i, j, k) with i <= j <= k, or -1 -1 -1 for an empty slot; every such triple of blocks 0 to 15 stands in exactly one row; the live slots of a device come first; some device has all 6 slots live.
All inputs are finite; a program needn't handle non-finite values.
Results may differ from the reference program's by a relative error of at most 0.0037.
Values may be sent and summed in bfloat16 or wider, within the bound.
A program may use at most 128 MiB of HBM per device.

```python
import jax
import jax.numpy as jnp
import numpy as np
from jax import lax

N = 1024
NB = 16
R = 48
BS = 64
NUNIQ = 816
SLOTS = 6
DEVICES = 256


def draw_ownership(key, part):
    listing = np.array([[lead_block, mid_block, tail_block] for lead_block in range(NB) for mid_block in range(lead_block, NB) for tail_block in range(mid_block, NB)], dtype=np.int32)
    shuffled = jnp.asarray(listing)[jax.random.permutation(jax.random.fold_in(key, 11), listing.shape[0])]
    ranking = jax.random.permutation(jax.random.fold_in(key, 12), DEVICES)
    base_load = NUNIQ // DEVICES
    extra_load = NUNIQ % DEVICES
    loads = base_load + (ranking < extra_load).astype(jnp.int32) + jnp.where(ranking % 2 == 0, base_load - 1, 1 - base_load)
    offsets = jnp.cumsum(loads) - loads
    slot_ids = jnp.arange(SLOTS, dtype=jnp.int32)
    wanted = offsets[:, None] + slot_ids[None, :]
    live = slot_ids[None, :] < loads[:, None]
    selected_rows = shuffled[jnp.clip(wanted, 0, NUNIQ - 1)]
    return jnp.where(live[:, :, None], selected_rows, -1).reshape(DEVICES * SLOTS, 3).astype(jnp.int32)


def block_levels(stream_key, shape, pieces, smallest, largest):
    level = 1.0
    for dim, blocks in pieces:
        draws = jax.random.uniform(jax.random.fold_in(jax.random.fold_in(stream_key, 6), dim), (blocks,), jnp.float32, smallest / len(pieces), largest / len(pieces))
        level = level * jnp.repeat(jnp.exp(draws), shape[dim] // blocks).reshape((-1,) + (1,) * (len(shape) - 1 - dim))
    return level


def scatter_about(stream_key, dims, deviation, most, pieces=(), kind=jnp.bfloat16):
    values = deviation * jax.random.normal(stream_key, dims, jnp.float32)
    if pieces:
        values = values * block_levels(stream_key, dims, pieces, -0.22, 0.18)
    return jnp.clip(values, -most, most).astype(kind)


def setup_inputs(seed: int = 0) -> dict:
    arg_keys = jax.random.split(jax.random.key(seed), 4)
    blocks = scatter_about(arg_keys[0], (DEVICES * SLOTS, BS, BS * BS), 1.0, 6.0, ((0, 256),))
    ownership = draw_ownership(jax.random.fold_in(arg_keys[3], 71), 0)
    basis_rows = scatter_about(arg_keys[2], (N, R), N ** -0.5, 0.1875)
    return dict(blocks=blocks, ownership=ownership, basis_rows=basis_rows)


ORDERS = ((0, 1, 2), (0, 2, 1), (1, 0, 2), (1, 2, 0), (2, 0, 1), (2, 1, 0))
REDUCE_FORMS = ("gxyz,gxq->gyzq", "gxyz,gyq->gxzq", "gxyz,gzq->gxyq")


def unpack(stored, unique_triples):
    number = stored.shape[0]
    extent = stored.shape[1]
    unpacked = stored.reshape(number, extent, extent, extent)
    leading_block_index = lax.broadcasted_iota(jnp.int32, (1, extent, extent, extent), 1)
    middle = lax.broadcasted_iota(jnp.int32, (1, extent, extent, extent), 2)
    trailing = lax.broadcasted_iota(jnp.int32, (1, extent, extent, extent), 3)
    same_front = (unique_triples[:, 0] == unique_triples[:, 1])[:, None, None, None]
    same_back = (unique_triples[:, 1] == unique_triples[:, 2])[:, None, None, None]

    def order_back(values):
        return jnp.where(middle <= trailing, values, jnp.swapaxes(values, 2, 3))

    def order_front(values):
        return jnp.where(leading_block_index <= middle, values, jnp.swapaxes(values, 1, 2))

    unpacked = jnp.where(same_back, order_back(unpacked), unpacked)
    unpacked = jnp.where(same_front, order_front(unpacked), unpacked)
    unpacked = jnp.where(same_back, order_back(unpacked), unpacked)
    return unpacked


def slot_terms(stored, unique_triples, basis_rows):
    extent = stored.shape[1]
    columns = basis_rows.shape[1]
    unpacked = unpack(stored, unique_triples).astype(jnp.float32)
    basis_blocks = basis_rows.reshape(basis_rows.shape[0] // extent, extent, columns)
    selected_rows = jnp.take(basis_blocks, jnp.clip(unique_triples, 0, basis_blocks.shape[0] - 1), axis=0).astype(jnp.float32)
    factors = (selected_rows[:, 0], selected_rows[:, 1], selected_rows[:, 2])
    reduced = [jnp.einsum(REDUCE_FORMS[slot_pos], unpacked, factors[slot_pos]).astype(jnp.bfloat16).astype(jnp.float32) for slot_pos in range(3)]
    by_row = [0.0, 0.0, 0.0]
    for position in range(6):
        row_slot_index, middle_slot_index, last_slot = ORDERS[position]
        contraction_form = "zixl,zxo->ziol" if row_slot_index < middle_slot_index else "hwie,hwy->hiye"
        contrib = jnp.einsum(contraction_form, reduced[last_slot], factors[middle_slot_index])
        ordered = unique_triples[:, jnp.array(ORDERS[position])]
        distinct = unique_triples[:, 0] >= 0
        for earlier in ORDERS[:position]:
            distinct = distinct & jnp.any(ordered != unique_triples[:, jnp.array(earlier)], axis=1)
        by_row[row_slot_index] = by_row[row_slot_index] + jnp.where(distinct[:, None, None, None], contrib, 0.0)
    stacked = jnp.stack(by_row, axis=1)
    return stacked.reshape(stacked.shape[0], 3, extent, columns * columns)


def reference(blocks, ownership, basis_rows):
    extent = N // NB
    per_turn = 16
    turns = blocks.shape[0] // per_turn
    stored_all = blocks.reshape(turns, per_turn, extent, extent * extent)
    owned_all = ownership.reshape(turns, per_turn, 3)

    def scan_step(accumulated, scan_item):
        stored, unique_triples = scan_item
        contribs = slot_terms(stored, unique_triples, basis_rows)
        targets = jnp.clip(unique_triples, 0, NB - 1).reshape(-1).astype(jnp.int32)
        accumulated = accumulated.at[targets].add(contribs.reshape(-1, extent, R * R))
        return accumulated, None

    zero_rows = jnp.zeros((NB, extent, R * R), jnp.float32)
    summed, _ = lax.scan(scan_step, zero_rows, (stored_all, owned_all))
    product = summed.reshape(N, R, R)
    symmetric = (0.5 * (product + jnp.swapaxes(product, 1, 2))).reshape(N, R * R)
    rounded = symmetric.astype(jnp.bfloat16)
    return jnp.dot(rounded, rounded.T, preferred_element_type=jnp.float32) / R
```

```python
import jax
import jax.numpy as jnp
from jax import lax
from jax.experimental import pallas as pl
from jax.experimental.pallas import tpu as pltpu
from jax.sharding import Mesh
from jax.sharding import PartitionSpec as P

N, NB, R, BS = 1024, 16, 48, 64
PITCH = 56
PQ = 1536


def turned(tile):
    return pltpu.roll(tile, BS, 1)


def contract_kernel(own, blk, ut, keep, send, sbuf, vv, ww, acc):
    slot = pl.program_id(0)
    slots = pl.num_programs(0)

    @pl.when(slot == 0)
    def _():
        def clear(t, carry):
            acc[t] = jnp.zeros((R * R, 128), jnp.float32)
            return carry

        lax.fori_loop(0, 8, clear, 0)

    i, j, k = own[slot * 3], own[slot * 3 + 1], own[slot * 3 + 2]

    @pl.when(i >= 0)
    def _():
        low = lax.broadcasted_iota(jnp.int32, (R, 128), 1) < BS
        halves = lax.broadcasted_iota(jnp.int32, (R, 128), 1) >> 6
        sbuf[...] = blk[0]

        @pl.when((i == j) | (j == k))
        def _():
            front, back = i == j, j == k

            def weigh(c, carry):
                at = pl.ds(pl.multiple_of(c * 128, 128), 128)
                lane = lax.broadcasted_iota(jnp.int32, (BS, 128), 1)
                x = lax.broadcasted_iota(jnp.int32, (BS, 128), 0)
                y = 2 * c + (lane >> 6)
                z = lane & 63
                f1 = jnp.where(x < y, 1.0, jnp.where(x == y, 0.5, 0.0))
                f2 = jnp.where(y < z, 1.0, jnp.where(y == z, 0.5, 0.0))
                f1 = jnp.where(front, f1, 1.0)
                f2 = jnp.where(back, f2, 1.0)
                f = f1 * f2
                f = jnp.where(f == 0.25, 1.0 / 6.0, f)
                sbuf[:, at] = (blk[0, :, at].astype(jnp.float32) * f).astype(jnp.bfloat16)
                return carry

            lax.fori_loop(0, 32, weigh, 0)

        ui, uj, uk = ut[i], ut[j], ut[k]
        ukz = jnp.concatenate([uk, jnp.zeros((R, BS), jnp.bfloat16)], axis=1)

        for c in range(8):
            v = jnp.dot(ui, sbuf[:, c * 512 : (c + 1) * 512], preferred_element_type=jnp.float32)
            for t in range(4):
                tile = v[:, t * 128 : (t + 1) * 128]
                other = turned(tile)
                y = 2 * (4 * c + t)
                vv[y * PITCH : y * PITCH + R, :] = jnp.where(low, tile, other)
                vv[(y + 1) * PITCH : (y + 1) * PITCH + R, :] = jnp.where(low, other, tile)
        for c in range(16):
            both = jnp.concatenate(
                [sbuf[:, c * 128 : (c + 1) * 128], sbuf[:, (c + 16) * 128 : (c + 17) * 128]], axis=0
            ).T
            both = jnp.concatenate([both[:BS], both[BS:]], axis=1)
            v = jnp.dot(uk, both, preferred_element_type=jnp.float32)
            for t in range(2):
                tile = v[:, t * 128 : (t + 1) * 128]
                other = turned(tile)
                y = 2 * c + t
                ww[y * PITCH : y * PITCH + R, :] = jnp.where(low, tile, other)
                ww[(y + 32) * PITCH : (y + 32) * PITCH + R, :] = jnp.where(low, other, tile)

        keep_i = halves == (i & 1)
        keep_j = halves == (j & 1)
        keep_k = halves == (k & 1)

        def add(row_block, keep, first, tile):
            at = pl.ds(first * R, R)
            acc[row_block >> 1, at, :] += jnp.where(keep, tile, 0.0)

        for g in range(12):
            parts = [
                vv[pl.ds(4 * g + t, BS, stride=PITCH), :].astype(jnp.bfloat16) for t in range(4)
            ]
            zk = jnp.dot(uj, jnp.concatenate(parts, axis=1), preferred_element_type=jnp.float32)
            zj = lax.dot_general(
                ukz,
                jnp.concatenate(parts, axis=0),
                (((1,), (1,)), ((), ())),
                preferred_element_type=jnp.float32,
            )
            for t in range(4):
                add(k, keep_k, 4 * g + t, zk[:, t * 128 : (t + 1) * 128])
            for t in range(2):
                tile = zj[:, t * 128 : (t + 1) * 128]
                other = turned(tile)
                add(j, keep_j, 4 * g + 2 * t, jnp.where(low, tile, other))
                add(j, keep_j, 4 * g + 2 * t + 1, jnp.where(low, other, tile))
            parts = [
                ww[pl.ds(4 * g + t, BS, stride=PITCH), :].astype(jnp.bfloat16) for t in range(4)
            ]
            zi = jnp.dot(uj, jnp.concatenate(parts, axis=1), preferred_element_type=jnp.float32)
            for t in range(4):
                add(i, keep_i, 4 * g + t, zi[:, t * 128 : (t + 1) * 128])

    @pl.when(slot == slots - 1)
    def _():
        core = lax.axis_index("gx_1")

        def pack(y, carry):
            for out, t in ((keep, 2 * y + core), (send, 2 * y + 1 - core)):
                at = 0
                for p in range(R):
                    first = p // 16 * 16
                    rows = R - first
                    plain = acc[t, p * R + first : (p + 1) * R, :]
                    swapped = acc.at[t][pl.ds(first * R + p, rows, stride=R), :]
                    out[y, at : at + rows, :] = (plain + swapped).astype(out.dtype)
                    at += rows
            return carry

        lax.fori_loop(0, 4, pack, 0)


def local_terms(blocks, ownership, basis_t):
    slots = blocks.shape[0]
    return pl.pallas_call(
        contract_kernel,
        grid_spec=pltpu.PrefetchScalarGridSpec(
            num_scalar_prefetch=1,
            grid=(slots,),
            in_specs=[
                pl.BlockSpec((1, BS, BS * BS), lambda s, own: (s, 0, 0)),
                pl.BlockSpec((NB, R, BS), lambda s, own: (0, 0, 0)),
            ],
            out_specs=[pl.BlockSpec((4, PQ, 128), lambda s, own: (0, 0, 0))] * 2,
            scratch_shapes=[
                pltpu.VMEM((BS, BS * BS), jnp.bfloat16),
                pltpu.VMEM((BS * PITCH, 128), jnp.float32),
                pltpu.VMEM((BS * PITCH, 128), jnp.float32),
                pltpu.VMEM((8, R * R, 128), jnp.float32),
            ],
        ),
        out_shape=[
            jax.ShapeDtypeStruct((4, PQ, 128), jnp.float32),
            jax.ShapeDtypeStruct((4, PQ, 128), jnp.bfloat16),
        ],
        compiler_params=pltpu.CompilerParams(
            dimension_semantics=("arbitrary",), vmem_limit_bytes=48 * 1024 * 1024
        ),
        name="contract",
    )(ownership.reshape(-1), blocks, basis_t)


MESH = pl.DeviceIdType.MESH
NY, NC, NZ, NX = 4, 2, 8, 4
F32, BF16 = jnp.float32, jnp.bfloat16


def exchange_kernel(
    keep,
    give,
    out,
    r1,
    e,
    r2a,
    r2b,
    fa,
    fb,
    r3a,
    r3b,
    g,
    g32,
    r4,
    h,
    yg,
    pb,
    r6,
    s1,
    q1,
    s2a,
    q2a,
    s2b,
    q2b,
    s3a,
    q3a,
    s3b,
    q3b,
    s4,
    q4,
    s5,
    q5,
    s6,
    q6,
):
    y, c, z, x = (lax.axis_index(a) for a in ("gx_0", "gx_1", "gy", "gz"))
    me = (y * NC + c) * NX + x
    half = NZ // 2

    def at_y(v):
        return (v, c, z, x)

    def at_x(v):
        return (y, c, z, v)

    def at_z(v):
        return (y, c, v, x)

    def in_plane(p):
        return (p // (NC * NX), (p // NX) % NC, z, p % NX)

    def around(v, o, n):
        return lax.rem(v + o, n)

    def remote(src, dst, send, recv, where):
        return pltpu.make_async_remote_copy(
            src_ref=src, dst_ref=dst, send_sem=send, recv_sem=recv, device_id=where, device_id_type=MESH
        )

    barrier = pltpu.get_barrier_semaphore()

    def greet_plane(o, carry):
        pl.semaphore_signal(
            barrier, inc=1, device_id=in_plane(around(me, o, 32)), device_id_type=MESH
        )
        return carry

    def greet_z(o, carry):
        pl.semaphore_signal(barrier, inc=1, device_id=at_z(around(z, o, NZ)), device_id_type=MESH)
        return carry

    lax.fori_loop(1, 32, greet_plane, 0)
    lax.fori_loop(1, NZ, greet_z, 0)
    pl.semaphore_wait(barrier, 31 + NZ - 1)

    def swap(k):
        part = pl.ds(k * half, half)
        return remote(
            give.at[:, part], r1.at[:, part], s1.at[k], q1.at[k], (y, 1 - c, z, x)
        )

    for k in range(2):
        swap(k).start()

    def add_pair(v, k):
        def body(t, carry):
            zz = k * half + t
            e[v, zz] = (keep[v, zz] + r1[v, zz].astype(F32)).astype(BF16)
            return carry

        lax.fori_loop(0, half, body, 0)

    def send2a(o):
        v = around(y, o, NY)
        return remote(e.at[v, pl.ds(0, half)], r2a.at[y], s2a.at[v], q2a.at[y], at_y(v))

    def got2a(o):
        v = around(y, o, NY)
        return remote(e.at[v, pl.ds(0, half)], r2a.at[v], s2a.at[v], q2a.at[v], at_y(v))

    def send2b(o):
        v = around(x, o, NX)
        return remote(e.at[:, pl.ds(half, half), v], r2b.at[x], s2b.at[v], q2b.at[x], at_x(v))

    def got2b(o):
        v = around(x, o, NX)
        return remote(e.at[:, pl.ds(half, half), v], r2b.at[v], s2b.at[v], q2b.at[v], at_x(v))

    swap(0).wait_recv()
    for o in (2, 1, 3):
        add_pair(around(y, o, NY), 0)
        send2a(o).start()
    swap(1).wait_recv()

    def add_all(v, carry):
        add_pair(v, 1)
        return carry

    lax.fori_loop(0, NY, add_all, 0)
    for o in (2, 1, 3):
        send2b(o).start()

    def send3a(o):
        v = around(x, o, NX)
        return remote(fa.at[:, v], r3a.at[x], s3a.at[v], q3a.at[x], at_x(v))

    def got3a(o):
        v = around(x, o, NX)
        return remote(fa.at[:, v], r3a.at[v], s3a.at[v], q3a.at[v], at_x(v))

    def send3b(o):
        v = around(y, o, NY)
        return remote(fb.at[v], r3b.at[y], s3b.at[v], q3b.at[y], at_y(v))

    def got3b(o):
        v = around(y, o, NY)
        return remote(fb.at[v], r3b.at[v], s3b.at[v], q3b.at[v], at_y(v))

    for o in (1, 3, 2):
        got2a(o).wait_recv()

    def add_a(t, carry):
        total = keep[y, t] + r1[y, t].astype(F32)
        for o in (1, 2, 3):
            total += r2a[around(y, o, NY), t].astype(F32)
        fa[t] = total
        return carry

    lax.fori_loop(0, half, add_a, 0)
    for o in (2, 1, 3):
        send3a(o).start()
    for o in (1, 3, 2):
        got2b(o).wait_recv()

    def add_b(t, carry):
        v, zz = t // half, lax.rem(t, half)
        total = keep[v, half + zz, x] + r1[v, half + zz, x].astype(F32)
        for o in (1, 2, 3):
            total += r2b[around(x, o, NX), v, zz].astype(F32)
        fb[v, zz] = total
        return carry

    lax.fori_loop(0, NY * half, add_b, 0)
    for o in (2, 1, 3):
        send3b(o).start()

    for o in (1, 3, 2):
        got3a(o).wait_recv()
    for o in (1, 3, 2):
        got3b(o).wait_recv()

    def add_c(t, carry):
        total = fa[t, x]
        for o in (1, 2, 3):
            total += r3a[around(x, o, NX), t]
        g32[t] = total
        g[t] = total.astype(BF16)
        total = fb[y, t]
        for o in (1, 2, 3):
            total += r3b[around(y, o, NY), t]
        g32[half + t] = total
        g[half + t] = total.astype(BF16)
        return carry

    lax.fori_loop(0, half, add_c, 0)

    def send4(o):
        v = around(z, o, NZ)
        return remote(g.at[v], r4.at[z], s4.at[v], q4.at[z], at_z(v))

    def got4(o):
        v = around(z, o, NZ)
        return remote(g.at[v], r4.at[v], s4.at[v], q4.at[v], at_z(v))

    for o in (4, 3, 5, 2, 6, 1, 7):
        send4(o).start()
    total = g32[z]
    for o in (1, 7, 2, 6, 3, 5, 4):
        got4(o).wait_recv()
        total += r4[around(z, o, NZ)].astype(F32)
    rows = total.astype(BF16)
    h[...] = rows
    yg[me] = rows

    def send5(o):
        p = around(me, o, 32)
        return remote(h, yg.at[me], s5.at[p], q5.at[me], in_plane(p))

    def got5(o):
        p = around(me, o, 32)
        return remote(h, yg.at[p], s5.at[p], q5.at[p], in_plane(p))

    def start5(o, carry):
        send5(o).start()
        return carry

    def wait5(o, carry):
        got5(o).wait_recv()
        return carry

    lax.fori_loop(1, 32, start5, 0)
    lax.fori_loop(1, 32, wait5, 0)

    weighted = []
    for t in range(12):
        tile = z * 12 + t
        w = jnp.where(
            tile < 48,
            1.0 if t % 3 == 0 else 2.0,
            jnp.where(tile < 80, 1.0 if t % 2 == 0 else 2.0, 1.0),
        )
        rows = yg[(y * NC + c) * NX + t // 3, (t % 3) * 16 : (t % 3 + 1) * 16]
        weighted.append((rows.astype(F32) * w).astype(BF16))
    weighted = jnp.concatenate(weighted, axis=0)
    row = lax.broadcasted_iota(jnp.int32, (64, 128), 0)
    lane = lax.broadcasted_iota(jnp.int32, (64, 128), 1)
    chosen = ((row >> 3) * 16 + 4 * x + (row & 7) == lane) & ((row & 7) < 4)
    left = lax.dot_general(
        chosen.astype(F32).astype(BF16),
        weighted,
        (((1,), (1,)), ((), ())),
        preferred_element_type=F32,
    ).astype(BF16)
    for t in range(8):
        right = jnp.concatenate([yg[4 * t + v] for v in range(4)], axis=0)
        part = jnp.dot(left, right, preferred_element_type=F32)
        for v in range(NZ):
            pb[v, :, t * 128 : (t + 1) * 128] = part[8 * v : 8 * v + 4]

    def send6(o):
        v = around(z, o, NZ)
        return remote(pb.at[v], r6.at[z], s6.at[v], q6.at[z], at_z(v))

    def got6(o):
        v = around(z, o, NZ)
        return remote(pb.at[v], r6.at[v], s6.at[v], q6.at[v], at_z(v))

    for o in (4, 3, 5, 2, 6, 1, 7):
        send6(o).start()
    total = pb[z]
    for o in (1, 7, 2, 6, 3, 5, 4):
        got6(o).wait_recv()
        total += r6[around(z, o, NZ)]
    out[...] = total / R

    for k in range(2):
        swap(k).wait_send()
    for o in (1, 2, 3):
        send2a(o).wait_send()
        send2b(o).wait_send()
        send3a(o).wait_send()
        send3b(o).wait_send()
    for o in range(1, NZ):
        send4(o).wait_send()
        send6(o).wait_send()

    def end5(o, carry):
        send5(o).wait_send()
        return carry

    lax.fori_loop(1, 32, end5, 0)


def summed_gram(keep, give):
    keep, give = (v.reshape(NY, NZ, NX, R, 128) for v in (keep, give))
    dma = pltpu.SemaphoreType.DMA
    half = NZ // 2
    return pl.pallas_call(
        exchange_kernel,
        out_shape=jax.ShapeDtypeStruct((4, 1024), F32),
        in_specs=[pl.BlockSpec(memory_space=pltpu.VMEM)] * 2,
        out_specs=pl.BlockSpec(memory_space=pltpu.VMEM),
        scratch_shapes=[
            pltpu.VMEM((NY, NZ, NX, R, 128), BF16),
            pltpu.VMEM((NY, NZ, NX, R, 128), BF16),
            pltpu.VMEM((NY, half, NX, R, 128), BF16),
            pltpu.VMEM((NX, NY, half, R, 128), BF16),
            pltpu.VMEM((half, NX, R, 128), F32),
            pltpu.VMEM((NY, half, R, 128), F32),
            pltpu.VMEM((NX, half, R, 128), F32),
            pltpu.VMEM((NY, half, R, 128), F32),
            pltpu.VMEM((NZ, R, 128), BF16),
            pltpu.VMEM((NZ, R, 128), F32),
            pltpu.VMEM((NZ, R, 128), BF16),
            pltpu.VMEM((R, 128), BF16),
            pltpu.VMEM((32, R, 128), BF16),
            pltpu.VMEM((NZ, 4, 1024), F32),
            pltpu.VMEM((NZ, 4, 1024), F32),
            dma((2,)),
            dma((2,)),
            dma((NY,)),
            dma((NY,)),
            dma((NX,)),
            dma((NX,)),
            dma((NX,)),
            dma((NX,)),
            dma((NY,)),
            dma((NY,)),
            dma((NZ,)),
            dma((NZ,)),
            dma((32,)),
            dma((32,)),
            dma((NZ,)),
            dma((NZ,)),
        ],
        compiler_params=pltpu.CompilerParams(
            collective_id=0, has_side_effects=True, vmem_limit_bytes=40 * 1024 * 1024
        ),
        name="exchange",
    )(keep, give)

GX_GY_GZ = ("gx_0", "gx_1", "gy", "gz")


def local(blocks, ownership, basis_rows):
    basis_t = basis_rows.reshape(NB, BS, R).swapaxes(1, 2)
    return summed_gram(*local_terms(blocks, ownership, basis_t))


def solution(mesh):
    split = Mesh(
        mesh.devices.reshape(4, 2, mesh.shape["gy"], mesh.shape["gz"]), GX_GY_GZ
    )
    return jax.shard_map(
        local,
        mesh=split,
        in_specs=(P(GX_GY_GZ, None, None), P(GX_GY_GZ, None), P()),
        out_specs=P(GX_GY_GZ, None),
        check_vma=False,
    )
```

```python
import jax
import jax.numpy as jnp
from jax import lax
from jax.experimental import pallas as pl
from jax.experimental.pallas import tpu as pltpu
from jax.sharding import Mesh
from jax.sharding import PartitionSpec as P

N, NB, R, BS = 1024, 16, 48, 64
PITCH = 56
PQ = 1536


def turned(tile):
    return pltpu.roll(tile, BS, 1)


def contract_kernel(owned, stored, factors, keep, send, own, basis, blk, small, sems, ut, sbuf, vv, ww, acc):
    slots = stored.shape[0]

    def fetch(s):
        return pltpu.make_async_copy(stored.at[s], blk.at[s], sems.at[s])

    own_copy = pltpu.make_async_copy(owned, own, small.at[0])
    basis_copy = pltpu.make_async_copy(factors, basis, small.at[1])
    own_copy.start()
    basis_copy.start()
    for s in range(slots):
        fetch(s).start()

    def clear(t, carry):
        acc[t] = jnp.zeros(acc.shape[1:], jnp.float32)
        return carry

    lax.fori_loop(0, 8, clear, 0)
    own_copy.wait()
    basis_copy.wait()
    for v in range(NB):
        ut[v] = basis[:, v * BS : (v + 1) * BS]

    def add_slot(slot, carry):
        fetch(slot).wait()
        contract_slot(own, blk.at[slot], ut, sbuf, vv, ww, acc, slot)
        return carry

    lax.fori_loop(0, slots, add_slot, 0)

    core = lax.axis_index("gx_1")

    def pack(y, carry):
        for out, t in ((keep, 2 * y + core), (send, 2 * y + 1 - core)):
            at = 0
            for p in range(R):
                first = p // 16 * 16
                rows = R - first
                plain = acc[t, p * PITCH + first : p * PITCH + R, :]
                swapped = acc.at[t][pl.ds(first * PITCH + p, rows, stride=PITCH), :]
                out[y, at : at + rows, :] = (plain + swapped).astype(out.dtype)
                at += rows
        return carry

    lax.fori_loop(0, 4, pack, 0)


def contract_slot(own, blk, ut, sbuf, vv, ww, acc, slot):
    i, j, k = own[0, slot], own[1, slot], own[2, slot]

    @pl.when(i >= 0)
    def _():
        low = lax.broadcasted_iota(jnp.int32, (R, 128), 1) < BS
        halves = lax.broadcasted_iota(jnp.int32, (R, 128), 1) >> 6
        front, back = i == j, j == k
        lane = lax.broadcasted_iota(jnp.int32, (BS, 128), 1)
        x = lax.broadcasted_iota(jnp.int32, (BS, 128), 0)
        upper, z = lane >> 6, lane & 63

        @pl.when(~(front | back))
        def _():
            sbuf[...] = blk[...]

        @pl.when(front ^ back)
        def _():
            def halves_of(n):
                return (0.5 * n.astype(jnp.float32) + 0.5).astype(jnp.bfloat16)

            def least(equal):
                shape = jnp.full((BS, 128), jnp.where(equal, 0.0, 1.0), jnp.float32)
                return shape.astype(jnp.bfloat16)

            xy, yz = halves_of(upper - x), halves_of(z - upper)
            xy_least, yz_least = least(front), least(back)
            one = jnp.ones((BS, 128), jnp.bfloat16)
            for c in range(32):
                f1 = jnp.minimum(jnp.maximum(xy + jnp.bfloat16(c), xy_least), one)
                f2 = jnp.minimum(jnp.maximum(yz - jnp.bfloat16(c), yz_least), one)
                sbuf[:, c * 128 : (c + 1) * 128] = blk[:, c * 128 : (c + 1) * 128] * (f1 * f2)

        @pl.when(front & back)
        def _():
            def weigh(c, carry):
                at = pl.ds(pl.multiple_of(c * 128, 128), 128)
                y = 2 * c + upper
                f1 = jnp.where(x < y, 1.0, jnp.where(x == y, 0.5, 0.0))
                f2 = jnp.where(y < z, 1.0, jnp.where(y == z, 0.5, 0.0))
                f = f1 * f2
                f = jnp.where(f == 0.25, 1.0 / 6.0, f)
                sbuf[:, at] = (blk[:, at].astype(jnp.float32) * f).astype(jnp.bfloat16)
                return carry

            lax.fori_loop(0, 32, weigh, 0)

        ui, uj, uk = ut[i], ut[j], ut[k]
        ukz = jnp.concatenate([uk, jnp.zeros((R, BS), jnp.bfloat16)], axis=1)

        for c in range(8):
            v = jnp.dot(ui, sbuf[:, c * 512 : (c + 1) * 512], preferred_element_type=jnp.float32)
            for t in range(4):
                tile = v[:, t * 128 : (t + 1) * 128]
                other = turned(tile)
                y = 2 * (4 * c + t)
                vv[y * PITCH : y * PITCH + R, :] = jnp.where(low, tile, other)
                vv[(y + 1) * PITCH : (y + 1) * PITCH + R, :] = jnp.where(low, other, tile)
        for c in range(16):
            both = jnp.concatenate(
                [sbuf[:, c * 128 : (c + 1) * 128], sbuf[:, (c + 16) * 128 : (c + 17) * 128]], axis=0
            ).T
            both = jnp.concatenate([both[:BS], both[BS:]], axis=1)
            v = jnp.dot(uk, both, preferred_element_type=jnp.float32)
            for t in range(2):
                tile = v[:, t * 128 : (t + 1) * 128]
                other = turned(tile)
                y = 2 * c + t
                ww[y * PITCH : y * PITCH + R, :] = jnp.where(low, tile, other)
                ww[(y + 32) * PITCH : (y + 32) * PITCH + R, :] = jnp.where(low, other, tile)

        keep_i = halves == (i & 1)
        keep_j = halves == (j & 1)
        keep_k = halves == (k & 1)

        def add(row_block, keep, first, tile):
            at = pl.ds(first * PITCH, R)
            acc[row_block >> 1, at, :] += jnp.where(keep, tile, 0.0)

        for g in range(12):
            parts = [
                vv[pl.ds(4 * g + t, BS, stride=PITCH), :].astype(jnp.bfloat16) for t in range(4)
            ]
            zk = jnp.dot(uj, jnp.concatenate(parts, axis=1), preferred_element_type=jnp.float32)
            zj = lax.dot_general(
                ukz,
                jnp.concatenate(parts, axis=0),
                (((1,), (1,)), ((), ())),
                preferred_element_type=jnp.float32,
            )
            for t in range(4):
                add(k, keep_k, 4 * g + t, zk[:, t * 128 : (t + 1) * 128])
            for t in range(2):
                tile = zj[:, t * 128 : (t + 1) * 128]
                other = turned(tile)
                add(j, keep_j, 4 * g + 2 * t, jnp.where(low, tile, other))
                add(j, keep_j, 4 * g + 2 * t + 1, jnp.where(low, other, tile))
            parts = [
                ww[pl.ds(4 * g + t, BS, stride=PITCH), :].astype(jnp.bfloat16) for t in range(4)
            ]
            zi = jnp.dot(uj, jnp.concatenate(parts, axis=1), preferred_element_type=jnp.float32)
            for t in range(4):
                add(i, keep_i, 4 * g + t, zi[:, t * 128 : (t + 1) * 128])


def local_terms(blocks, ownership, basis_rows):
    slots = blocks.shape[0]
    return pl.pallas_call(
        contract_kernel,
        in_specs=[
            pl.BlockSpec(memory_space=pltpu.HBM),
            pl.BlockSpec(memory_space=pltpu.HBM),
            pl.BlockSpec(memory_space=pltpu.HBM),
        ],
        out_specs=[pl.BlockSpec(memory_space=pltpu.VMEM)] * 2,
        scratch_shapes=[
            pltpu.SMEM((3, slots), jnp.int32),
            pltpu.VMEM((R, N), jnp.bfloat16),
            pltpu.VMEM((slots, BS, BS * BS), jnp.bfloat16),
            pltpu.SemaphoreType.DMA((2,)),
            pltpu.SemaphoreType.DMA((slots,)),
            pltpu.VMEM((NB, R, BS), jnp.bfloat16),
            pltpu.VMEM((BS, BS * BS), jnp.bfloat16),
            pltpu.VMEM((BS * PITCH, 128), jnp.float32),
            pltpu.VMEM((BS * PITCH, 128), jnp.float32),
            pltpu.VMEM((8, R * PITCH, 128), jnp.float32),
        ],
        out_shape=[
            jax.ShapeDtypeStruct((4, PQ, 128), jnp.float32),
            jax.ShapeDtypeStruct((4, PQ, 128), jnp.bfloat16),
        ],
        compiler_params=pltpu.CompilerParams(vmem_limit_bytes=48 * 1024 * 1024),
        name="contract",
    )(ownership.T, blocks, basis_rows.T)


MESH = pl.DeviceIdType.MESH
NY, NC, NZ, NX = 4, 2, 8, 4
F32, BF16 = jnp.float32, jnp.bfloat16


def exchange_kernel(
    keep,
    give,
    out,
    r1,
    e,
    r2a,
    r2b,
    fa,
    fb,
    r3a,
    r3b,
    g,
    g32,
    r4,
    h,
    yg,
    pb,
    r6,
    s1,
    q1,
    s2a,
    q2a,
    s2b,
    q2b,
    s3a,
    q3a,
    s3b,
    q3b,
    s4,
    q4,
    s5,
    q5,
    s6,
    q6,
):
    y, c, z, x = (lax.axis_index(a) for a in ("gx_0", "gx_1", "gy", "gz"))
    me = (y * NC + c) * NX + x
    half = NZ // 2

    def at_y(v):
        return (v, c, z, x)

    def at_x(v):
        return (y, c, z, v)

    def at_z(v):
        return (y, c, v, x)

    def in_plane(p):
        return (p // (NC * NX), (p // NX) % NC, z, p % NX)

    def around(v, o, n):
        return lax.rem(v + o, n)

    def remote(src, dst, send, recv, where):
        return pltpu.make_async_remote_copy(
            src_ref=src, dst_ref=dst, send_sem=send, recv_sem=recv, device_id=where, device_id_type=MESH
        )

    barrier = pltpu.get_barrier_semaphore()

    def greet_plane(o, carry):
        pl.semaphore_signal(
            barrier, inc=1, device_id=in_plane(around(me, o, 32)), device_id_type=MESH
        )
        return carry

    def greet_z(o, carry):
        pl.semaphore_signal(barrier, inc=1, device_id=at_z(around(z, o, NZ)), device_id_type=MESH)
        return carry

    lax.fori_loop(1, 32, greet_plane, 0)
    lax.fori_loop(1, NZ, greet_z, 0)
    pl.semaphore_wait(barrier, 31 + NZ - 1)

    def swap(k):
        part = pl.ds(k * half, half)
        return remote(
            give.at[:, part], r1.at[:, part], s1.at[k], q1.at[k], (y, 1 - c, z, x)
        )

    for k in range(2):
        swap(k).start()

    def add_pair(v, k):
        def body(t, carry):
            zz = k * half + t
            e[v, zz] = (keep[v, zz] + r1[v, zz].astype(F32)).astype(BF16)
            return carry

        lax.fori_loop(0, half, body, 0)

    def send2a(o):
        v = around(y, o, NY)
        return remote(e.at[v, pl.ds(0, half)], r2a.at[y], s2a.at[v], q2a.at[y], at_y(v))

    def got2a(o):
        v = around(y, o, NY)
        return remote(e.at[v, pl.ds(0, half)], r2a.at[v], s2a.at[v], q2a.at[v], at_y(v))

    def send2b(o):
        v = around(x, o, NX)
        return remote(e.at[:, pl.ds(half, half), v], r2b.at[x], s2b.at[v], q2b.at[x], at_x(v))

    def got2b(o):
        v = around(x, o, NX)
        return remote(e.at[:, pl.ds(half, half), v], r2b.at[v], s2b.at[v], q2b.at[v], at_x(v))

    swap(0).wait_recv()
    for o in (2, 1, 3):
        add_pair(around(y, o, NY), 0)
        send2a(o).start()
    swap(1).wait_recv()

    def add_all(v, carry):
        add_pair(v, 1)
        return carry

    lax.fori_loop(0, NY, add_all, 0)
    for o in (2, 1, 3):
        send2b(o).start()

    def send3a(o):
        v = around(x, o, NX)
        return remote(fa.at[:, v], r3a.at[x], s3a.at[v], q3a.at[x], at_x(v))

    def got3a(o):
        v = around(x, o, NX)
        return remote(fa.at[:, v], r3a.at[v], s3a.at[v], q3a.at[v], at_x(v))

    def send3b(o):
        v = around(y, o, NY)
        return remote(fb.at[v], r3b.at[y], s3b.at[v], q3b.at[y], at_y(v))

    def got3b(o):
        v = around(y, o, NY)
        return remote(fb.at[v], r3b.at[v], s3b.at[v], q3b.at[v], at_y(v))

    for o in (1, 3, 2):
        got2a(o).wait_recv()

    def add_a(t, carry):
        total = keep[y, t] + r1[y, t].astype(F32)
        for o in (1, 2, 3):
            total += r2a[around(y, o, NY), t].astype(F32)
        fa[t] = total
        return carry

    lax.fori_loop(0, half, add_a, 0)
    for o in (2, 1, 3):
        send3a(o).start()
    for o in (1, 3, 2):
        got2b(o).wait_recv()

    def add_b(t, carry):
        v, zz = t // half, lax.rem(t, half)
        total = keep[v, half + zz, x] + r1[v, half + zz, x].astype(F32)
        for o in (1, 2, 3):
            total += r2b[around(x, o, NX), v, zz].astype(F32)
        fb[v, zz] = total
        return carry

    lax.fori_loop(0, NY * half, add_b, 0)
    for o in (2, 1, 3):
        send3b(o).start()

    for o in (1, 3, 2):
        got3a(o).wait_recv()
    for o in (1, 3, 2):
        got3b(o).wait_recv()

    def add_c(t, carry):
        total = fa[t, x]
        for o in (1, 2, 3):
            total += r3a[around(x, o, NX), t]
        g32[t] = total
        g[t] = total.astype(BF16)
        total = fb[y, t]
        for o in (1, 2, 3):
            total += r3b[around(y, o, NY), t]
        g32[half + t] = total
        g[half + t] = total.astype(BF16)
        return carry

    lax.fori_loop(0, half, add_c, 0)

    def send4(o):
        v = around(z, o, NZ)
        return remote(g.at[v], r4.at[z], s4.at[v], q4.at[z], at_z(v))

    def got4(o):
        v = around(z, o, NZ)
        return remote(g.at[v], r4.at[v], s4.at[v], q4.at[v], at_z(v))

    for o in (4, 3, 5, 2, 6, 1, 7):
        send4(o).start()
    total = g32[z]
    for o in (1, 7, 2, 6, 3, 5, 4):
        got4(o).wait_recv()
        total += r4[around(z, o, NZ)].astype(F32)
    rows = total.astype(BF16)
    h[...] = rows
    yg[me] = rows

    def send5(o):
        p = around(me, o, 32)
        return remote(h, yg.at[me], s5.at[p], q5.at[me], in_plane(p))

    def got5(o):
        p = around(me, o, 32)
        return remote(h, yg.at[p], s5.at[p], q5.at[p], in_plane(p))

    def start5(o, carry):
        send5(o).start()
        return carry

    def wait5(o, carry):
        got5(o).wait_recv()
        return carry

    lax.fori_loop(1, 32, start5, 0)
    lax.fori_loop(1, 32, wait5, 0)

    weighted = []
    for t in range(12):
        tile = z * 12 + t
        w = jnp.where(
            tile < 48,
            1.0 if t % 3 == 0 else 2.0,
            jnp.where(tile < 80, 1.0 if t % 2 == 0 else 2.0, 1.0),
        )
        rows = yg[(y * NC + c) * NX + t // 3, (t % 3) * 16 : (t % 3 + 1) * 16]
        weighted.append((rows.astype(F32) * w).astype(BF16))
    weighted = jnp.concatenate(weighted, axis=0)
    row = lax.broadcasted_iota(jnp.int32, (64, 128), 0)
    lane = lax.broadcasted_iota(jnp.int32, (64, 128), 1)
    chosen = ((row >> 3) * 16 + 4 * x + (row & 7) == lane) & ((row & 7) < 4)
    left = lax.dot_general(
        chosen.astype(F32).astype(BF16),
        weighted,
        (((1,), (1,)), ((), ())),
        preferred_element_type=F32,
    ).astype(BF16)
    for t in range(8):
        right = jnp.concatenate([yg[4 * t + v] for v in range(4)], axis=0)
        part = jnp.dot(left, right, preferred_element_type=F32)
        for v in range(NZ):
            pb[v, :, t * 128 : (t + 1) * 128] = part[8 * v : 8 * v + 4]

    def send6(o):
        v = around(z, o, NZ)
        return remote(pb.at[v], r6.at[z], s6.at[v], q6.at[z], at_z(v))

    def got6(o):
        v = around(z, o, NZ)
        return remote(pb.at[v], r6.at[v], s6.at[v], q6.at[v], at_z(v))

    for o in (4, 3, 5, 2, 6, 1, 7):
        send6(o).start()
    total = pb[z]
    for o in (1, 7, 2, 6, 3, 5, 4):
        got6(o).wait_recv()
        total += r6[around(z, o, NZ)]
    out[...] = total / R

    for k in range(2):
        swap(k).wait_send()
    for o in (1, 2, 3):
        send2a(o).wait_send()
        send2b(o).wait_send()
        send3a(o).wait_send()
        send3b(o).wait_send()
    for o in range(1, NZ):
        send4(o).wait_send()
        send6(o).wait_send()

    def end5(o, carry):
        send5(o).wait_send()
        return carry

    lax.fori_loop(1, 32, end5, 0)


def summed_gram(keep, give):
    keep, give = (v.reshape(NY, NZ, NX, R, 128) for v in (keep, give))
    dma = pltpu.SemaphoreType.DMA
    half = NZ // 2
    return pl.pallas_call(
        exchange_kernel,
        out_shape=jax.ShapeDtypeStruct((4, 1024), F32),
        in_specs=[pl.BlockSpec(memory_space=pltpu.VMEM)] * 2,
        out_specs=pl.BlockSpec(memory_space=pltpu.VMEM),
        scratch_shapes=[
            pltpu.VMEM((NY, NZ, NX, R, 128), BF16),
            pltpu.VMEM((NY, NZ, NX, R, 128), BF16),
            pltpu.VMEM((NY, half, NX, R, 128), BF16),
            pltpu.VMEM((NX, NY, half, R, 128), BF16),
            pltpu.VMEM((half, NX, R, 128), F32),
            pltpu.VMEM((NY, half, R, 128), F32),
            pltpu.VMEM((NX, half, R, 128), F32),
            pltpu.VMEM((NY, half, R, 128), F32),
            pltpu.VMEM((NZ, R, 128), BF16),
            pltpu.VMEM((NZ, R, 128), F32),
            pltpu.VMEM((NZ, R, 128), BF16),
            pltpu.VMEM((R, 128), BF16),
            pltpu.VMEM((32, R, 128), BF16),
            pltpu.VMEM((NZ, 4, 1024), F32),
            pltpu.VMEM((NZ, 4, 1024), F32),
            dma((2,)),
            dma((2,)),
            dma((NY,)),
            dma((NY,)),
            dma((NX,)),
            dma((NX,)),
            dma((NX,)),
            dma((NX,)),
            dma((NY,)),
            dma((NY,)),
            dma((NZ,)),
            dma((NZ,)),
            dma((32,)),
            dma((32,)),
            dma((NZ,)),
            dma((NZ,)),
        ],
        compiler_params=pltpu.CompilerParams(
            collective_id=0, has_side_effects=True, vmem_limit_bytes=40 * 1024 * 1024
        ),
        name="exchange",
    )(keep, give)

GX_GY_GZ = ("gx_0", "gx_1", "gy", "gz")


def local(blocks, ownership, basis_rows):
    return summed_gram(*local_terms(blocks, ownership, basis_rows))


def solution(mesh):
    split = Mesh(
        mesh.devices.reshape(4, 2, mesh.shape["gy"], mesh.shape["gz"]), GX_GY_GZ
    )
    return jax.shard_map(
        local,
        mesh=split,
        in_specs=(P(GX_GY_GZ, None, None), P(GX_GY_GZ, None), P()),
        out_specs=P(GX_GY_GZ, None),
        check_vma=False,
    )
```

```python
import jax
import jax.numpy as jnp
from jax import lax
from jax.experimental import pallas as pl
from jax.experimental.pallas import tpu as pltpu
from jax.sharding import Mesh
from jax.sharding import PartitionSpec as P

N, NB, R, BS = 1024, 16, 48, 64
PITCH = 56
AB, DG = 1024, 256


def turned(tile):
    return pltpu.roll(tile, BS, 1)


def contract_kernel(
    owned, stored, factors, keep, keep_d, send, send_d, own, basis, blk, small, sems, ut, sbuf, vv, ww, acc
):
    slots = stored.shape[0]

    def fetch(s):
        return pltpu.make_async_copy(stored.at[s], blk.at[s], sems.at[s])

    own_copy = pltpu.make_async_copy(owned, own, small.at[0])
    basis_copy = pltpu.make_async_copy(factors, basis, small.at[1])
    own_copy.start()
    basis_copy.start()
    for s in range(slots):
        fetch(s).start()

    def clear(t, carry):
        acc[t] = jnp.zeros(acc.shape[1:], jnp.float32)
        return carry

    lax.fori_loop(0, 8, clear, 0)
    own_copy.wait()
    basis_copy.wait()
    for v in range(NB):
        ut[v] = basis[:, v * BS : (v + 1) * BS]

    def add_slot(slot, carry):
        fetch(slot).wait()
        contract_slot(own, blk.at[slot], ut, sbuf, vv, ww, acc, slot)
        return carry

    lax.fori_loop(0, slots, add_slot, 0)

    core = lax.axis_index("gx_1")

    def pack(y, carry):
        for out, out_d, t in ((keep, keep_d, 2 * y + core), (send, send_d, 2 * y + 1 - core)):

            def rows_of(p, first, count):
                plain = acc[t, p * PITCH + first : p * PITCH + first + count, :]
                swapped = acc.at[t][pl.ds(first * PITCH + p, count, stride=PITCH), :]
                return plain + swapped

            at = 0
            for p in range(0, R - 8, 2):
                first = p // 8 * 8 + 8
                both = [rows_of(v, first, R - first) for v in (p, p + 1)]
                both = jnp.concatenate(both, axis=0)
                out[y, at : at + both.shape[0], :] = both.astype(out.dtype)
                at += both.shape[0]
            rest = [
                2.0 * acc.at[t][pl.ds((16 * v + 8) * (PITCH + 1), 8, stride=PITCH + 1), :]
                for v in range(3)
            ]
            rest = jnp.concatenate(rest + [jnp.zeros((AB - at - 24, 128), jnp.float32)], axis=0)
            out[y, at:AB, :] = rest.astype(out.dtype)
            row = lax.broadcasted_iota(jnp.int32, (8, 128), 0)
            for v in range(3):
                for a in range(0, 8, 2):
                    both = []
                    for b in (a, a + 1):
                        upper = rows_of(16 * v + b, 16 * v, 8)
                        lower = rows_of(16 * v + 8 + b, 16 * v + 8, 8)
                        both.append(jnp.where(row >= b, upper, lower))
                    at = (8 * v + a) * 8
                    both = jnp.concatenate(both, axis=0)
                    out_d[y, at : at + 16, :] = both.astype(out.dtype)
            out_d[y, 192:, :] = jnp.zeros((64, 128), out.dtype)
        return carry

    lax.fori_loop(0, 4, pack, 0)


def contract_slot(own, blk, ut, sbuf, vv, ww, acc, slot):
    i, j, k = own[0, slot], own[1, slot], own[2, slot]

    @pl.when(i >= 0)
    def _():
        low = lax.broadcasted_iota(jnp.int32, (R, 128), 1) < BS
        halves = lax.broadcasted_iota(jnp.int32, (R, 128), 1) >> 6
        front, back = i == j, j == k
        lane = lax.broadcasted_iota(jnp.int32, (BS, 128), 1)
        x = lax.broadcasted_iota(jnp.int32, (BS, 128), 0)
        upper, z = lane >> 6, lane & 63

        @pl.when(~(front | back))
        def _():
            sbuf[...] = blk[...]

        @pl.when(front ^ back)
        def _():
            def halves_of(n):
                return (0.5 * n.astype(jnp.float32) + 0.5).astype(jnp.bfloat16)

            def least(equal):
                shape = jnp.full((BS, 128), jnp.where(equal, 0.0, 1.0), jnp.float32)
                return shape.astype(jnp.bfloat16)

            xy, yz = halves_of(upper - x), halves_of(z - upper)
            xy_least, yz_least = least(front), least(back)
            one = jnp.ones((BS, 128), jnp.bfloat16)
            for c in range(32):
                f1 = jnp.minimum(jnp.maximum(xy + jnp.bfloat16(c), xy_least), one)
                f2 = jnp.minimum(jnp.maximum(yz - jnp.bfloat16(c), yz_least), one)
                sbuf[:, c * 128 : (c + 1) * 128] = blk[:, c * 128 : (c + 1) * 128] * (f1 * f2)

        @pl.when(front & back)
        def _():
            def weigh(c, carry):
                at = pl.ds(pl.multiple_of(c * 128, 128), 128)
                y = 2 * c + upper
                f1 = jnp.where(x < y, 1.0, jnp.where(x == y, 0.5, 0.0))
                f2 = jnp.where(y < z, 1.0, jnp.where(y == z, 0.5, 0.0))
                f = f1 * f2
                f = jnp.where(f == 0.25, 1.0 / 6.0, f)
                sbuf[:, at] = (blk[:, at].astype(jnp.float32) * f).astype(jnp.bfloat16)
                return carry

            lax.fori_loop(0, 32, weigh, 0)

        ui, uj, uk = ut[i], ut[j], ut[k]
        ukz = jnp.concatenate([uk, jnp.zeros((R, BS), jnp.bfloat16)], axis=1)

        for c in range(8):
            v = jnp.dot(ui, sbuf[:, c * 512 : (c + 1) * 512], preferred_element_type=jnp.float32)
            for t in range(4):
                tile = v[:, t * 128 : (t + 1) * 128]
                other = turned(tile)
                y = 2 * (4 * c + t)
                vv[y * PITCH : y * PITCH + R, :] = jnp.where(low, tile, other)
                vv[(y + 1) * PITCH : (y + 1) * PITCH + R, :] = jnp.where(low, other, tile)
        for c in range(16):
            both = jnp.concatenate(
                [sbuf[:, c * 128 : (c + 1) * 128], sbuf[:, (c + 16) * 128 : (c + 17) * 128]], axis=0
            ).T
            both = jnp.concatenate([both[:BS], both[BS:]], axis=1)
            v = jnp.dot(uk, both, preferred_element_type=jnp.float32)
            for t in range(2):
                tile = v[:, t * 128 : (t + 1) * 128]
                other = turned(tile)
                y = 2 * c + t
                ww[y * PITCH : y * PITCH + R, :] = jnp.where(low, tile, other)
                ww[(y + 32) * PITCH : (y + 32) * PITCH + R, :] = jnp.where(low, other, tile)

        keep_i = halves == (i & 1)
        keep_j = halves == (j & 1)
        keep_k = halves == (k & 1)

        def add(row_block, keep, first, tile):
            at = pl.ds(first * PITCH, R)
            acc[row_block >> 1, at, :] += jnp.where(keep, tile, 0.0)

        for g in range(12):
            parts = [
                vv[pl.ds(4 * g + t, BS, stride=PITCH), :].astype(jnp.bfloat16) for t in range(4)
            ]
            zk = jnp.dot(uj, jnp.concatenate(parts, axis=1), preferred_element_type=jnp.float32)
            zj = lax.dot_general(
                ukz,
                jnp.concatenate(parts, axis=0),
                (((1,), (1,)), ((), ())),
                preferred_element_type=jnp.float32,
            )
            for t in range(4):
                add(k, keep_k, 4 * g + t, zk[:, t * 128 : (t + 1) * 128])
            for t in range(2):
                tile = zj[:, t * 128 : (t + 1) * 128]
                other = turned(tile)
                add(j, keep_j, 4 * g + 2 * t, jnp.where(low, tile, other))
                add(j, keep_j, 4 * g + 2 * t + 1, jnp.where(low, other, tile))
            parts = [
                ww[pl.ds(4 * g + t, BS, stride=PITCH), :].astype(jnp.bfloat16) for t in range(4)
            ]
            zi = jnp.dot(uj, jnp.concatenate(parts, axis=1), preferred_element_type=jnp.float32)
            for t in range(4):
                add(i, keep_i, 4 * g + t, zi[:, t * 128 : (t + 1) * 128])


def local_terms(blocks, ownership, basis_rows):
    slots = blocks.shape[0]
    return pl.pallas_call(
        contract_kernel,
        in_specs=[
            pl.BlockSpec(memory_space=pltpu.HBM),
            pl.BlockSpec(memory_space=pltpu.HBM),
            pl.BlockSpec(memory_space=pltpu.HBM),
        ],
        out_specs=[pl.BlockSpec(memory_space=pltpu.VMEM)] * 4,
        scratch_shapes=[
            pltpu.SMEM((3, slots), jnp.int32),
            pltpu.VMEM((R, N), jnp.bfloat16),
            pltpu.VMEM((slots, BS, BS * BS), jnp.bfloat16),
            pltpu.SemaphoreType.DMA((2,)),
            pltpu.SemaphoreType.DMA((slots,)),
            pltpu.VMEM((NB, R, BS), jnp.bfloat16),
            pltpu.VMEM((BS, BS * BS), jnp.bfloat16),
            pltpu.VMEM((BS * PITCH, 128), jnp.float32),
            pltpu.VMEM((BS * PITCH, 128), jnp.float32),
            pltpu.VMEM((8, R * PITCH, 128), jnp.float32),
        ],
        out_shape=[
            jax.ShapeDtypeStruct((4, AB, 128), jnp.float32),
            jax.ShapeDtypeStruct((4, DG, 128), jnp.float32),
            jax.ShapeDtypeStruct((4, AB, 128), jnp.bfloat16),
            jax.ShapeDtypeStruct((4, DG, 128), jnp.bfloat16),
        ],
        compiler_params=pltpu.CompilerParams(vmem_limit_bytes=48 * 1024 * 1024),
        name="contract",
    )(ownership.T, blocks, basis_rows.T)


MESH = pl.DeviceIdType.MESH
NY, NC, NZ, NX = 4, 2, 8, 4
HALF = NZ // 2
F32, BF16 = jnp.float32, jnp.bfloat16
T3, T6 = F32, F32
OFF4 = (2, 1, 3)
ON4 = (1, 3, 2)
OFF8 = (4, 3, 5, 2, 6, 1, 7)
ON8 = (1, 7, 2, 6, 3, 5, 4)


def exchange_kernel(
    keep,
    keep_d,
    give,
    give_d,
    out,
    r1,
    r1d,
    e,
    ed,
    r2a,
    r2b,
    r2d,
    fa,
    fb,
    fd,
    r3a,
    r3b,
    r3d,
    g,
    gd,
    r4,
    r4d,
    h,
    yg,
    pb,
    r6,
    own_a,
    own_b,
    s1,
    q1,
    s2a,
    q2a,
    s2b,
    q2b,
    s2d,
    q2d,
    s3a,
    q3a,
    s3b,
    q3b,
    s3d,
    q3d,
    s4,
    q4,
    s4d,
    q4d,
    s5,
    q5,
    s6,
    q6,
):
    y, c, z, x = (lax.axis_index(a) for a in ("gx_0", "gx_1", "gy", "gz"))
    me = (y * NC + c) * NX + x

    def at_y(v):
        return (v, c, z, x)

    def at_x(v):
        return (y, c, z, v)

    def at_z(v):
        return (y, c, v, x)

    def in_plane(p):
        return (p // (NC * NX), (p // NX) % NC, z, p % NX)

    def remote(src, dst, send, recv, where):
        return pltpu.make_async_remote_copy(
            src_ref=src, dst_ref=dst, send_sem=send, recv_sem=recv, device_id=where, device_id_type=MESH
        )

    def exchange(src_of, land, send, recv, own, n, where):
        def to(o):
            v = lax.rem(own + o, n)
            return remote(src_of(v), land.at[own], send.at[v], recv.at[own], where(v))

        def got(o):
            v = lax.rem(own + o, n)
            return remote(src_of(v), land.at[v], send.at[v], recv.at[v], where(v))

        return to, got

    def slot(own, o, n):
        return lax.rem(own + o, n)

    barrier = pltpu.get_barrier_semaphore()

    def greet_plane(o, carry):
        pl.semaphore_signal(
            barrier, inc=1, device_id=in_plane(lax.rem(me + o, 32)), device_id_type=MESH
        )
        return carry

    def greet_z(o, carry):
        pl.semaphore_signal(
            barrier, inc=1, device_id=at_z(lax.rem(z + o, NZ)), device_id_type=MESH
        )
        return carry

    lax.fori_loop(1, NZ, greet_z, 0)
    lax.fori_loop(1, 32, greet_plane, 0)
    pl.semaphore_wait(barrier, 31 + NZ - 1)

    other = (y, 1 - c, z, x)
    swap_a = remote(give.at[:, pl.ds(0, HALF)], r1.at[:, pl.ds(0, HALF)], s1.at[0], q1.at[0], other)
    swap_b = remote(
        give.at[:, pl.ds(HALF, HALF)], r1.at[:, pl.ds(HALF, HALF)], s1.at[1], q1.at[1], other
    )
    swap_d = remote(give_d, r1d, s1.at[2], q1.at[2], other)
    swap_a.start()
    swap_d.start()
    swap_b.start()

    to2a, got2a = exchange(
        lambda v: e.at[v, pl.ds(0, HALF)], r2a, s2a, q2a, y, NY, at_y
    )
    to2b, got2b = exchange(
        lambda v: e.at[:, pl.ds(HALF, HALF), v], r2b, s2b, q2b, x, NX, at_x
    )
    to2d, got2d = exchange(lambda v: ed.at[v], r2d, s2d, q2d, z, NZ, at_z)
    to3a, got3a = exchange(lambda v: fa.at[v], r3a, s3a, q3a, x, NX, at_x)
    to3b, got3b = exchange(lambda v: fb.at[v], r3b, s3b, q3b, y, NY, at_y)
    to3d, got3d = exchange(lambda v: fd.at[v], r3d, s3d, q3d, y, NY, at_y)
    to4, got4 = exchange(lambda v: g.at[v], r4, s4, q4, z, NZ, at_z)
    to4d, got4d = exchange(lambda v: gd.at[v], r4d, s4d, q4d, x, NX, at_x)
    to6, got6 = exchange(lambda v: pb.at[v], r6, s6, q6, z, NZ, at_z)

    def pair(v, zz):
        return keep[v, zz] + r1[v, zz].astype(F32)

    def pair_d(v, zz):
        return keep_d[v, zz] + r1d[v, zz].astype(F32)

    swap_a.wait_recv()
    for o in OFF4:
        v = slot(y, o, NY)

        def add_1a(t, carry):
            e[v, t] = pair(v, t).astype(BF16)
            return carry

        lax.fori_loop(0, HALF, add_1a, 0)
        to2a(o).start()
    swap_d.wait_recv()

    def add_1d(t, carry):
        for v in range(NY):
            ed[t, v] = pair_d(v, t).astype(BF16)
        return carry

    lax.fori_loop(0, NZ, add_1d, 0)
    for o in OFF8:
        to2d(o).start()
    swap_b.wait_recv()

    def add_1b(t, carry):
        v, zz = t // HALF, HALF + lax.rem(t, HALF)
        e[v, zz] = pair(v, zz).astype(BF16)
        return carry

    lax.fori_loop(0, NY * HALF, add_1b, 0)
    for o in OFF4:
        to2b(o).start()

    for o in ON4:
        got2a(o).wait_recv()

    def add_2a(t, carry):
        total = pair(y, t)
        for o in ON4:
            total += r2a[slot(y, o, NY), t].astype(F32)
        for v in range(NX):
            fa[v, t] = total[v].astype(T3)
        own_a[t] = total
        return carry

    lax.fori_loop(0, HALF, add_2a, 0)
    for o in OFF4:
        to3a(o).start()
    for o in ON4:
        got2b(o).wait_recv()

    def add_2b(t, carry):
        v, zz = t // HALF, lax.rem(t, HALF)
        total = keep[v, HALF + zz, x] + r1[v, HALF + zz, x].astype(F32)
        for o in ON4:
            total += r2b[slot(x, o, NX), v, zz].astype(F32)
        fb[v, zz] = total.astype(T3)
        own_b[v, zz] = total
        return carry

    lax.fori_loop(0, NY * HALF, add_2b, 0)
    for o in OFF4:
        to3b(o).start()
    for o in ON8:
        got2d(o).wait_recv()

    def add_2d(v, carry):
        total = pair_d(v, z)
        for o in ON8:
            total += r2d[slot(z, o, NZ), v].astype(F32)
        fd[v] = total
        return carry

    lax.fori_loop(0, NY, add_2d, 0)
    for o in OFF4:
        to3d(o).start()

    for o in ON4:
        got3a(o).wait_recv()
    mine = jnp.zeros((R - 16, 128), F32)

    def add_3a(t, mine):
        total = own_a[t, x]
        for o in ON4:
            total += r3a[slot(x, o, NX), t].astype(F32)
        g[t] = total.astype(BF16)
        return jnp.where(t == z, total, mine)

    mine = lax.fori_loop(0, HALF, add_3a, mine)
    for o in ON4:
        got3b(o).wait_recv()

    def add_3b(t, mine):
        total = own_b[y, t]
        for o in ON4:
            total += r3b[slot(y, o, NY), t].astype(F32)
        g[HALF + t] = total.astype(BF16)
        return jnp.where(HALF + t == z, total, mine)

    mine = lax.fori_loop(0, HALF, add_3b, mine)
    for o in OFF8:
        to4(o).start()
    for o in ON4:
        got3d(o).wait_recv()
    total = fd[y]
    for o in ON4:
        total += r3d[slot(y, o, NY)]
    for v in range(NX):
        gd[v] = total[8 * v : 8 * v + 8]
    for o in OFF4:
        to4d(o).start()
    for o in ON8:
        got4(o).wait_recv()
        mine += r4[slot(z, o, NZ)].astype(F32)
    total = gd[x]
    for o in ON4:
        got4d(o).wait_recv()
        total += r4d[slot(x, o, NX)]
    rows = jnp.concatenate([mine, total], axis=0).astype(BF16)
    h[...] = rows
    yg[me] = rows

    def send5(o):
        p = lax.rem(me + o, 32)
        return remote(h, yg.at[me], s5.at[p], q5.at[me], in_plane(p))

    def got5(o):
        p = lax.rem(me + o, 32)
        return remote(h, yg.at[p], s5.at[p], q5.at[p], in_plane(p))

    def start5(o, carry):
        send5(o).start()
        return carry

    def wait5(o, carry):
        got5(o).wait_recv()
        return carry

    lax.fori_loop(1, 32, start5, 0)
    lax.fori_loop(1, 32, wait5, 0)

    row = lax.broadcasted_iota(jnp.int32, (64, 128), 0)
    lane = lax.broadcasted_iota(jnp.int32, (64, 128), 1)
    chosen = ((row >> 3) * 16 + 4 * x + (row & 7) == lane) & ((row & 7) < 4)
    chosen = chosen.astype(F32).astype(BF16)
    line = lax.broadcasted_iota(jnp.int32, (40, 128), 0)
    parts = []
    for v in range(NX):
        own_x = yg[(y * NC + c) * NX + v].astype(F32)
        chunk = z * NX + v
        plain = jnp.where(chunk < 30, 2.0, 1.0)
        diagonal = 32 + lax.rem(z, 2) * 4 + v
        weight = jnp.where(line < 32, plain, jnp.where(line == diagonal, 1.0, 2.0))
        left = lax.dot_general(
            chosen,
            (own_x * weight).astype(BF16),
            (((1,), (1,)), ((), ())),
            preferred_element_type=F32,
        ).astype(BF16)
        right = jnp.concatenate([yg[NX * t + v] for t in range(8)], axis=1)
        parts.append(jnp.dot(left, right, preferred_element_type=F32))
    part = (parts[0] + parts[1]) + (parts[2] + parts[3])
    for v in range(NZ):
        pb[v] = part[8 * v : 8 * v + 4].astype(T6)

    for o in OFF8:
        to6(o).start()
    total = pb[z].astype(F32)
    for o in ON8:
        got6(o).wait_recv()
        total += r6[slot(z, o, NZ)].astype(F32)
    out[...] = total / R

    swap_a.wait_send()
    swap_b.wait_send()
    swap_d.wait_send()
    for o in ON4:
        for to in (to2a, to2b, to3a, to3b, to3d, to4d):
            to(o).wait_send()
    for o in ON8:
        for to in (to2d, to4, to6):
            to(o).wait_send()

    def end5(o, carry):
        send5(o).wait_send()
        return carry

    lax.fori_loop(1, 32, end5, 0)


def summed_gram(keep, keep_d, give, give_d):
    keep, give = (v.reshape(NY, NZ, NX, 32, 128) for v in (keep, give))
    keep_d, give_d = (v.reshape(NY, NZ, 32, 128) for v in (keep_d, give_d))
    dma = pltpu.SemaphoreType.DMA
    vmem = pltpu.VMEM
    return pl.pallas_call(
        exchange_kernel,
        out_shape=jax.ShapeDtypeStruct((4, 1024), F32),
        in_specs=[pl.BlockSpec(memory_space=vmem)] * 4,
        out_specs=pl.BlockSpec(memory_space=vmem),
        scratch_shapes=[
            vmem((NY, NZ, NX, 32, 128), BF16),
            vmem((NY, NZ, 32, 128), BF16),
            vmem((NY, NZ, NX, 32, 128), BF16),
            vmem((NZ, NY, 32, 128), BF16),
            vmem((NY, HALF, NX, 32, 128), BF16),
            vmem((NX, NY, HALF, 32, 128), BF16),
            vmem((NZ, NY, 32, 128), BF16),
            vmem((NX, HALF, 32, 128), T3),
            vmem((NY, HALF, 32, 128), T3),
            vmem((NY, 32, 128), F32),
            vmem((NX, HALF, 32, 128), T3),
            vmem((NY, HALF, 32, 128), T3),
            vmem((NY, 32, 128), F32),
            vmem((NZ, 32, 128), BF16),
            vmem((NX, 8, 128), F32),
            vmem((NZ, 32, 128), BF16),
            vmem((NX, 8, 128), F32),
            vmem((40, 128), BF16),
            vmem((32, 40, 128), BF16),
            vmem((NZ, 4, 1024), T6),
            vmem((NZ, 4, 1024), T6),
            vmem((HALF, NX, 32, 128), F32),
            vmem((NY, HALF, 32, 128), F32),
        ]
        + [dma((3,))] * 2
        + [dma((NY,))] * 2
        + [dma((NX,))] * 2
        + [dma((NZ,))] * 2
        + [dma((NX,))] * 2
        + [dma((NY,))] * 4
        + [dma((NZ,))] * 2
        + [dma((NX,))] * 2
        + [dma((32,))] * 2
        + [dma((NZ,))] * 2,
        compiler_params=pltpu.CompilerParams(
            collective_id=0, has_side_effects=True, vmem_limit_bytes=40 * 1024 * 1024
        ),
        name="exchange",
    )(keep, keep_d, give, give_d)

GX_GY_GZ = ("gx_0", "gx_1", "gy", "gz")


def local(blocks, ownership, basis_rows):
    return summed_gram(*local_terms(blocks, ownership, basis_rows))


def solution(mesh):
    split = Mesh(
        mesh.devices.reshape(4, 2, mesh.shape["gy"], mesh.shape["gz"]), GX_GY_GZ
    )
    return jax.shard_map(
        local,
        mesh=split,
        in_specs=(P(GX_GY_GZ, None, None), P(GX_GY_GZ, None), P()),
        out_specs=P(GX_GY_GZ, None),
        check_vma=False,
    )
```
